32 devices in a mesh: gx: 8 (over z, y), gy: 4 (over x, core).
Axes of the slice: x: 2, y: 2, z: 4, core: 2. Of those that a mesh axis runs over, the one named last changes fastest.
Arguments:
- innovations: float32 [65536, 128], P(('gy', 'gx')), may hold values from -6 to 6
- left_root: float32 [65536, 128], P(('gy', 'gx')), may hold values from -6 to 6
- left_second: float32 [65536, 128], P(('gy', 'gx')), may hold values from -6 to 6
- left_third: float32 [65536, 128], P(('gy', 'gx')), may hold values from -6 to 6
- left_fourth: float32 [65536, 128], P(('gy', 'gx')), may hold values from -6 to 6
- right_root: float32 [65536, 128], P(('gy', 'gx')), may hold values from -0.0008544922 to 0.0008544922
- right_second: float32 [65536, 128], P(('gy', 'gx')), may hold values from -0.0012207031 to 0.0012207031
- right_third: float32 [65536, 128], P(('gy', 'gx')), may hold values from -0.0017089844 to 0.0017089844
- right_fourth: float32 [65536, 128], P(('gy', 'gx')), may hold values from -0.0024414062 to 0.0024414062
Outputs:
- solved: float32 [65536, 128], P(('gy', 'gx'))
The draws below stay inside these ranges and needn't reach their ends.
All inputs are finite; a program needn't handle non-finite values.
Results may differ from the reference program's by a relative error of at most 0.0001.
Values sent between devices are 32-bit elements; how exact they have to be, the bound alone decides.
No kernel may reach another device: no remote copies, remote signals or barrier semaphores. Data moves between devices by JAX's collectives and lax.ppermute only.
A program may use at most 64 MiB of HBM per device.

```python
import jax
import jax.numpy as jnp
from jax import lax

RANK = 128
NRHS = 128
NROWS = 65536


def block_scale(key, dims, split, least, high):
    loudness, own = 1.0, jax.random.fold_in(key, 6)
    for axis_at, blocks in split:
        steps = jnp.exp(jax.random.uniform(jax.random.fold_in(own, axis_at), (blocks,), jnp.float32, least / len(split), high / len(split)))
        loudness = loudness * jnp.repeat(steps, dims[axis_at] // blocks).reshape([-1 if axis == axis_at else 1 for axis in range(len(dims))])
    return loudness


def centred(key, shape, deviation, most, split=(), kind=jnp.bfloat16):
    factor_of = block_scale(key, shape, split, -0.22, 0.18) if split else 1.0
    values = jax.random.normal(key, shape, jnp.float32) * deviation * factor_of
    return jnp.minimum(jnp.maximum(values, -most), most).astype(kind)


def setup_inputs(seed: int = 0) -> dict:
    seeds = jax.random.split(jax.random.key(seed), 10)
    return {
        "innovations": centred(seeds[0], (NROWS, NRHS), 1.0, 6.0, ((0, 32),), jnp.float32),
        "left_root": centred(seeds[1], (NROWS, RANK), 1.0, 6.0, ((0, 32),), jnp.float32),
        "left_second": centred(seeds[2], (NROWS, RANK), 1.0, 6.0, ((0, 32),), jnp.float32),
        "left_third": centred(seeds[3], (NROWS, RANK), 1.0, 6.0, ((0, 32),), jnp.float32),
        "left_fourth": centred(seeds[4], (NROWS, RANK), 1.0, 6.0, ((0, 32),), jnp.float32),
        "right_root": centred(seeds[5], (NROWS, RANK), (11 * RANK * NROWS // 2) ** -0.5, 0.0008544922, ((0, 32),), jnp.float32),
        "right_second": centred(seeds[6], (NROWS, RANK), (11 * RANK * NROWS // 4) ** -0.5, 0.0012207031, ((0, 32),), jnp.float32),
        "right_third": centred(seeds[7], (NROWS, RANK), (11 * RANK * NROWS // 8) ** -0.5, 0.0017089844, ((0, 32),), jnp.float32),
        "right_fourth": centred(seeds[8], (NROWS, RANK), (11 * RANK * NROWS // 16) ** -0.5, 0.0024414062, ((0, 32),), jnp.float32),
    }


def reference(innovations, left_root, left_second, left_third, left_fourth, right_root, right_second, right_third, right_fourth):
    lefts = [left_root, left_second, left_third, left_fourth]
    rights = [right_root, right_second, right_third, right_fourth]
    total = innovations.shape[0]
    current = innovations
    highest = lax.Precision.HIGHEST
    for depth in (3, 2, 1, 0):
        kids = 2 ** (depth + 1)
        size = total // kids
        basis = lefts[depth].reshape(kids, size, RANK)
        weight = rights[depth].reshape(kids, size, RANK)
        columns = jnp.concatenate([current] + lefts[:depth], axis=1)
        width = columns.shape[1]
        blocks = columns.reshape(kids, size, width)
        own = jnp.einsum('kir,kis->krs', weight, basis, precision=highest)
        proj = jnp.einsum('kir,kic->krc', weight, blocks, precision=highest)
        own = own.reshape(kids // 2, 2, RANK, RANK)
        proj = proj.reshape(kids // 2, 2, RANK, width)
        identity = jnp.broadcast_to(jnp.eye(RANK, dtype=jnp.float32), (kids // 2, RANK, RANK))
        upper = jnp.concatenate([identity, own[:, 1]], axis=2)
        lower = jnp.concatenate([own[:, 0], identity], axis=2)
        system = jnp.concatenate([upper, lower], axis=1)
        target = jnp.concatenate([proj[:, 1], proj[:, 0]], axis=1)
        coeff = jnp.linalg.solve(system, target).reshape(kids, RANK, width)
        blocks = blocks - jnp.einsum('kir,krc->kic', basis, coeff, precision=highest)
        columns = blocks.reshape(total, width)
        current = columns[:, :NRHS]
        for level in range(depth):
            lefts[level] = columns[:, NRHS + level * RANK:NRHS + (level + 1) * RANK]
    return current
```

```python
import functools

import jax
import jax.numpy as jnp
from jax import lax
from jax.experimental import pallas as pl
from jax.experimental.pallas import tpu as pltpu
from jax.sharding import PartitionSpec as P


F32 = jnp.float32
BF16 = jnp.bfloat16
VMEM = pl.BlockSpec(memory_space=pltpu.VMEM)


def halves(value):
    high = value.astype(BF16)
    low = (value - high.astype(F32)).astype(BF16)
    return high, low


def dot(first, second, contract=1):
    return lax.dot_general(
        first, second, (((contract,), (0,)), ((), ())), preferred_element_type=F32
    )


def mul(first, second):
    width = second.shape[1]
    high, low = halves(second)
    left = jnp.concatenate(halves(first), axis=1)
    right = jnp.concatenate([high, low], axis=1)
    both = dot(left, jnp.concatenate([right, right], axis=0))
    return both[:, :width] + both[:, width:]


def identity(rank):
    rows = lax.broadcasted_iota(jnp.int32, (rank, rank), 0)
    cols = lax.broadcasted_iota(jnp.int32, (rank, rank), 1)
    return jnp.where(rows == cols, 1.0, 0.0).astype(F32)


def eliminate(matrix, right):
    rank = matrix.shape[0]
    rows = lax.broadcasted_iota(jnp.int32, (rank, 1), 0)
    lanes = lax.broadcasted_iota(jnp.int32, (rank, rank), 1)

    def step(k, carry):
        left, side = carry
        column = jnp.sum(jnp.where(lanes == k, left, 0.0), axis=1, keepdims=True)
        size = jnp.where(rows >= k, jnp.abs(column), -1.0)
        best = jnp.max(size, axis=0, keepdims=True)
        pivot = jnp.min(jnp.where(size == best, rows, rank), axis=0, keepdims=True)
        chosen = rows == pivot
        here = rows == k

        def row_of(mask, value):
            return jnp.sum(jnp.where(mask, value, 0.0), axis=0, keepdims=True)

        scale = 1.0 / row_of(chosen, column)
        left_row, side_row = row_of(chosen, left), row_of(chosen, side)
        left_old, side_old = row_of(here, left), row_of(here, side)
        moved = jnp.where(chosen, row_of(here, column), column)
        factor = jnp.where(here, 0.0, moved * scale)
        left = jnp.where(chosen, left_old, left) - factor * left_row
        side = jnp.where(chosen, side_old, side) - factor * side_row
        left = jnp.where(here, left_row * scale, left)
        side = jnp.where(here, side_row * scale, side)
        return left, side

    return lax.fori_loop(0, rank, step, (matrix, right))[1]


def solve_pair(own, other, inverse_ref):
    rank = own.shape[0]
    own_core, own_proj = own[:, :rank], own[:, rank:]
    other_core, other_proj = other[:, :rank], other[:, rank:]
    eye = identity(rank)
    product = mul(other_core, own_core)
    target = other_proj - mul(other_core, own_proj)
    square = mul(product, product)
    fourth = mul(square, square)
    guess = eye + product
    guess = guess + mul(guess, square)
    guess = guess + mul(guess, fourth)
    residual = eye - (guess - mul(product, guess))
    inverse_ref[...] = guess + mul(guess, residual)
    size = jnp.sum(residual * residual)

    @pl.when(jnp.logical_not(size < 1e-7))
    def _():
        inverse_ref[...] = eliminate(eye - product, eye)

    own_coeff = mul(inverse_ref[...], target)
    other_coeff = own_proj - mul(own_core, own_coeff)
    return own_coeff, other_coeff


def gram_kernel(*refs, weights, rank):
    out_ref = refs[-1]
    step = pl.program_id(0)

    @pl.when(step == 0)
    def _():
        out_ref[...] = jnp.zeros_like(out_ref)

    columns = jnp.concatenate([ref[...] for ref in refs[weights:-1]], axis=1)
    high, low = halves(columns)
    for at in range(weights):
        left_high, left_low = halves(refs[at][...])
        both = dot(jnp.concatenate([left_high, left_low], axis=1), high, 0)
        total = both[:rank] + both[rank:] + dot(left_high, low, 0)
        out_ref[at * rank : (at + 1) * rank, :] += total


def gram(weights, columns, chunk):
    rows, rank = weights[0].shape
    spec = pl.BlockSpec((chunk, rank), lambda i: (i, 0))
    shape = (rank * len(weights), sum(c.shape[1] for c in columns))
    return pl.pallas_call(
        functools.partial(gram_kernel, weights=len(weights), rank=rank),
        grid=(rows // chunk,),
        in_specs=[spec] * (len(weights) + len(columns)),
        out_specs=pl.BlockSpec(shape, lambda i: (0, 0)),
        out_shape=jax.ShapeDtypeStruct(shape, F32),
        compiler_params=pltpu.CompilerParams(vmem_limit_bytes=32 * 2**20),
    )(*weights, *columns)


def solve_kernel(own_ref, other_ref, own_out, other_out, inverse_ref):
    own_out[...], other_out[...] = solve_pair(own_ref[...], other_ref[...], inverse_ref)


def solve(own, other):
    rank = own.shape[0]
    shape = jax.ShapeDtypeStruct((rank, own.shape[1] - rank), F32)
    return pl.pallas_call(
        solve_kernel,
        in_specs=[VMEM, VMEM],
        out_specs=[VMEM, VMEM],
        out_shape=[shape, shape],
        scratch_shapes=[pltpu.VMEM((rank, rank), F32)],
    )(own, other)


def reduced(gram_own, gram_other, coeff_own, coeff_other):
    rank = coeff_own.shape[0]
    own = gram_own[:, rank:] - mul(gram_own[:, :rank], coeff_own)
    other = gram_other[:, rank:] - mul(gram_other[:, :rank], coeff_other)
    return own + other


def reduce_kernel(gram_own, gram_other, coeff_own, coeff_other, out_ref):
    out_ref[...] = reduced(
        gram_own[...], gram_other[...], coeff_own[...], coeff_other[...]
    )


def reduce(gram_own, gram_other, coeff_own, coeff_other):
    rank = coeff_own.shape[0]
    shape = (gram_own.shape[0], gram_own.shape[1] - rank)
    return pl.pallas_call(
        reduce_kernel,
        in_specs=[VMEM] * 4,
        out_specs=VMEM,
        out_shape=jax.ShapeDtypeStruct(shape, F32),
    )(gram_own, gram_other, coeff_own, coeff_other)


def last_pair_kernel(own_ref, other_ref, coeff_out, next_out, inverse_ref):
    rank = inverse_ref.shape[0]
    own, other = own_ref[...], other_ref[...]
    own_coeff, other_coeff = solve_pair(own[:rank], other[:rank], inverse_ref)
    coeff_out[...] = own_coeff
    next_out[...] = reduced(own[rank:], other[rank:], own_coeff, other_coeff)


def solve_and_reduce(own, other, rank):
    width = own.shape[1] - rank
    shape = jax.ShapeDtypeStruct((rank, width), F32)
    return pl.pallas_call(
        last_pair_kernel,
        in_specs=[VMEM, VMEM],
        out_specs=[VMEM, VMEM],
        out_shape=[shape, shape],
        scratch_shapes=[pltpu.VMEM((rank, rank), F32)],
    )(own, other)


def finish_kernel(
    own_ref, other_ref, third_ref, second_ref, first_ref, x_ref, *refs, depths, rank
):
    left_refs, out_ref = refs[:depths], refs[depths]
    inverse_ref, high_ref, low_ref = refs[depths + 1 :]

    @pl.when(pl.program_id(0) == 0)
    def _():
        parts = [solve_pair(own_ref[...], other_ref[...], inverse_ref)[0]]
        for depth, ref in enumerate((first_ref, second_ref, third_ref), 1):
            coeff = ref[...]
            part = coeff[:, depth * rank :]
            for level in range(depth):
                block = coeff[:, (depth - 1 - level) * rank : (depth - level) * rank]
                part = part - mul(block, parts[level])
            parts.append(part)
        high, low = halves(jnp.concatenate(parts, axis=0))
        high_ref[...] = high
        low_ref[...] = low

    bases = jnp.concatenate([ref[...] for ref in left_refs], axis=1)
    base_high, base_low = halves(bases)
    pair = jnp.concatenate([high_ref[...], low_ref[...]], axis=1)
    both = dot(base_high, pair)
    count = x_ref.shape[1]
    moved = both[:, :count] + both[:, count:] + dot(base_low, high_ref[...])
    out_ref[...] = x_ref[...] - moved


def finish(own, other, coeffs, x, lefts, chunk):
    rank = own.shape[0]
    rows, count = x.shape
    spec = pl.BlockSpec((chunk, count), lambda i: (i, 0))
    left_spec = pl.BlockSpec((chunk, rank), lambda i: (i, 0))
    depths = len(lefts)
    return pl.pallas_call(
        functools.partial(finish_kernel, depths=depths, rank=rank),
        grid=(rows // chunk,),
        in_specs=[VMEM] * 5 + [spec] + [left_spec] * depths,
        out_specs=spec,
        out_shape=jax.ShapeDtypeStruct((rows, count), F32),
        scratch_shapes=[
            pltpu.VMEM((rank, rank), F32),
            pltpu.VMEM((rank * depths, count), BF16),
            pltpu.VMEM((rank * depths, count), BF16),
        ],
        compiler_params=pltpu.CompilerParams(vmem_limit_bytes=32 * 2**20),
    )(own, other, *coeffs, x, *lefts)


def body(
    innovations,
    left_root,
    left_second,
    left_third,
    left_fourth,
    right_root,
    right_second,
    right_third,
    right_fourth,
):
    inner_size = lax.axis_size("gx")
    inner_bits = inner_size.bit_length() - 1
    device_bits = inner_bits + lax.axis_size("gy").bit_length() - 1
    rank = left_root.shape[1]
    chunk = min(512, innovations.shape[0])
    depths = 4
    summed_bits = device_bits - depths

    def swapped(value, bit, mask=0):
        if bit < inner_bits:
            axis, flip = "gx", 2**bit | mask
        else:
            axis, flip = "gy", 2 ** (bit - inner_bits)
        pairs = [(source, source ^ flip) for source in range(lax.axis_size(axis))]
        return lax.ppermute(value, axis, pairs)

    def sibling(value, depth):
        bit = device_bits - 1 - depth
        mask = 2 ** (bit - 1) if 2 <= bit < inner_bits else 0
        return swapped(value, bit, mask)

    def child_sum(value):
        for bit in range(summed_bits):
            value = value + swapped(value, bit)
        return value

    columns = [left_fourth, left_third, left_second, left_root, innovations]
    fourth = child_sum(gram([right_fourth], columns, chunk))
    third = child_sum(gram([right_third], columns, chunk))
    outer = child_sum(gram([right_second, right_root], columns, chunk))

    fourth_own, fourth_other = solve(fourth, sibling(fourth, 3))
    third = reduce(third, sibling(third, 3), fourth_own, fourth_other)
    third_own, third_other = solve(third, sibling(third, 2))
    outer = reduce(outer, sibling(outer, 3), fourth_own, fourth_other)
    outer = reduce(outer, sibling(outer, 2), third_own, third_other)
    second_own, root = solve_and_reduce(outer, sibling(outer, 1), rank)
    return finish(
        root,
        sibling(root, 0),
        (fourth_own, third_own, second_own),
        innovations,
        [left_root, left_second, left_third, left_fourth],
        chunk,
    )


def solution(mesh):
    spec = P(("gy", "gx"), None)
    return jax.shard_map(
        body, mesh=mesh, in_specs=(spec,) * 9, out_specs=spec, check_vma=False
    )
```
